32 devices in a mesh: sfc: 8 (over z, x), grp: 4 (over y, core).
Axes of the slice: x: 2, y: 2, z: 4, core: 2. Of those that a mesh axis runs over, the one named last changes fastest.
Arguments:
- source: float32 [32, 16, 1024], P('sfc', None, 'grp'), may hold values from -8 to 8
- layer_counts: int32 [8], P('sfc'), may hold values from 1 to 4, 21 in all
Outputs:
- solution: float32 [32, 16, 1024], P('sfc', None, 'grp')
- residual: float32 [32, 16, 1024], P('sfc', None, 'grp')
- direction: float32 [32, 16, 1024], P('sfc', None, 'grp')
The draws below stay inside these ranges and needn't reach their ends.
Inputs may be any that keep to these rules, and one draw needn't show every extreme that they name: `layer_counts`: each entry counts the live leading slots of that index of sfc; they sum to 21, and at least one entry equals 4.
All inputs are finite; a program needn't handle non-finite values. No bound on the sum of `layer_counts` on one device may be relied on, other than what follows from the above.
Results may differ from the reference program's by a relative error of at most 0.00011.
Values sent between devices are 32-bit elements; how exact they have to be, the bound alone decides.
No kernel may reach another device: no remote copies, remote signals or barrier semaphores. Data moves between devices by JAX's collectives and lax.ppermute only.
A program may use at most 64 MiB of HBM per device.

```python
import math
import jax
import jax.numpy as jnp
import numpy as np

E = 16
H = 8
BCAP = 4
PRE_SWEEPS = 2
POST_SWEEPS = 2
COARSE_SWEEPS = 4
SLOTS = 32
LIVE = 21
N_SFC = 8
N_GRP = 4


def draw_source(key, part):
    shape = (BCAP * N_SFC, E, N_GRP * E * E)
    slot = jnp.arange(BCAP * N_SFC, dtype=jnp.float32)
    device = jnp.floor(slot / BCAP)
    rise = (1.0 + 2.0 * device / max(N_SFC - 1, 1))[:, None, None]
    values = jax.random.normal(key, shape, jnp.float32) * rise
    return jnp.clip(values, -8.0, 8.0)


def profile(amount, total, reach, lean):
    portions = [(1 << 20) // math.isqrt(grade ** lean) + 1 for grade in range(2, amount + 1)]
    rest, given = total - reach - (amount - 1), [1] * (amount - 1)
    while rest > 0:
        free = [i for i in range(amount - 1) if given[i] < reach]
        whole, remaining = sum([portions[i] for i in free]), rest
        for i in free:
            extra = min(reach - given[i], max(1, remaining * portions[i] // whole), rest)
            given[i] = given[i] + extra
            rest = rest - extra
    return np.array([reach] + given)


def uneven_parts(own_key, amount, total, reach, slope):
    if amount == 2:
        one = jax.random.randint(own_key, (), max(1, total - reach), min(reach, total - 1) + 1)
        return jnp.stack([one, total - one])
    tallies = jnp.asarray(profile(amount, total, reach, slope), jnp.int32)
    twos = (amount - 1) // 2
    giver, sink = tallies[1:1 + 2 * twos:2], tallies[2:2 + 2 * twos:2]
    slack = jnp.minimum(giver - 1, reach - sink)
    shifted = jax.random.randint(jax.random.fold_in(own_key, 1), (twos,), 0, 1 << 20) % (slack + 1)
    tallies = tallies.at[1:1 + 2 * twos:2].set(giver - shifted).at[2:2 + 2 * twos:2].set(sink + shifted)
    return tallies[jax.random.permutation(jax.random.fold_in(own_key, 2), amount)]


def setup_inputs(seed: int = 0) -> dict:
    keys = jax.random.split(jax.random.key(seed), 3)
    return {
        "source": draw_source(jax.random.fold_in(keys[2], 71), 0),
        "layer_counts": uneven_parts(keys[1], N_SFC, LIVE, BCAP, 2).astype(jnp.int32),
    }


OMEGA = 2.0 / 3.0


def laplace(field, counts, edge):
    n_dev, planes, width = field.shape
    zero_plane = jnp.zeros((1, 1, width), jnp.float32)
    last_index = (counts * edge - 1).astype(jnp.int32)
    last = jnp.take_along_axis(field, last_index[:, None, None], axis=1)
    first = field[:, :1]
    prev_last = jnp.concatenate([zero_plane, last[:-1]], axis=0)
    next_first = jnp.concatenate([first[1:], zero_plane], axis=0)
    below = jnp.concatenate([prev_last, field[:, :-1]], axis=1)
    above = jnp.concatenate([field[:, 1:], jnp.zeros((n_dev, 1, width), jnp.float32)], axis=1)
    plane = jnp.arange(planes, dtype=jnp.int32)
    at_last = (plane[None, :] == last_index[:, None])[:, :, None]
    above = above + jnp.where(at_last, next_first, 0.0)
    pad_rows = jnp.zeros((n_dev, planes, edge), jnp.float32)
    north = jnp.concatenate([field[:, :, edge:], pad_rows], axis=2)
    south = jnp.concatenate([pad_rows, field[:, :, :-edge]], axis=2)
    column = (jnp.arange(width, dtype=jnp.int32) % edge)[None, None, :]
    pad_col = jnp.zeros((n_dev, planes, 1), jnp.float32)
    up_z = jnp.where(column != edge - 1, jnp.concatenate([field[:, :, 1:], pad_col], axis=2), 0.0)
    down_z = jnp.where(column != 0, jnp.concatenate([pad_col, field[:, :, :-1]], axis=2), 0.0)
    total = 6.0 * field - below - above - north - south - up_z - down_z
    live = (plane[None, :] < (counts * edge)[:, None])[:, :, None]
    return jnp.where(live, total, 0.0)


def restrict(field):
    n_dev, planes, width = field.shape
    across = width // (E * E) * E
    blocks = field.reshape(n_dev, planes // 2, 2, across // 2, 2, H, 2)
    return 0.125 * jnp.sum(blocks, axis=(2, 4, 6)).reshape(n_dev, planes // 2, (across // 2) * H)


def prolong(coarse):
    n_dev, planes, width = coarse.shape
    across = width // H
    blocks = coarse.reshape(n_dev, planes, 1, across, 1, H, 1)
    blocks = jnp.broadcast_to(blocks, (n_dev, planes, 2, across, 2, H, 2))
    return blocks.reshape(n_dev, planes * 2, across * 2 * H * 2)


def vcycle(rhs, counts):
    step = OMEGA / 6.0
    smooth = step * rhs
    for sweep in range(PRE_SWEEPS - 1):
        smooth = smooth + step * (rhs - laplace(smooth, counts, E))
    defect = rhs - laplace(smooth, counts, E)
    coarse_rhs = restrict(defect)
    coarse_step = OMEGA / 1.5
    correction = coarse_step * coarse_rhs
    for sweep in range(COARSE_SWEEPS - 1):
        correction = correction + coarse_step * (coarse_rhs - 0.25 * laplace(correction, counts, H))
    smooth = smooth + prolong(correction)
    for sweep in range(POST_SWEEPS):
        smooth = smooth + step * (rhs - laplace(smooth, counts, E))
    return smooth


def reference(source, layer_counts):
    width = source.shape[2]
    field = source.reshape(N_SFC, BCAP * E, width)
    plane = jnp.arange(BCAP * E, dtype=jnp.int32)
    live = (plane[None, :] < (layer_counts * E)[:, None])[:, :, None]
    first_rhs = jnp.where(live, field, 0.0)
    first_z = vcycle(first_rhs, layer_counts)
    image = laplace(first_z, layer_counts, E)
    rz_value = jnp.sum(first_rhs * first_z)
    curv = jnp.sum(first_z * image)
    alpha = rz_value / curv
    solution = alpha * first_z
    residual = first_rhs - alpha * image
    next_z = vcycle(residual, layer_counts)
    cross = jnp.sum(next_z * image)
    direction = next_z - (cross / curv) * first_z
    shape = (SLOTS, E, width)
    return solution.reshape(shape), residual.reshape(shape), direction.reshape(shape)
```

```python
import functools

import jax
import jax.numpy as jnp
from jax import lax
from jax.experimental import pallas as pl
from jax.experimental.pallas import tpu as pltpu
from jax.sharding import PartitionSpec as P

PRE_SWEEPS = 2
POST_SWEEPS = 2
COARSE_SWEEPS = 4
OMEGA = 2.0 / 3.0
LANES = 128
ROWS = 8


def halo_depth():
    def down_even(plane):
        return plane + plane % 2

    def cycle(reach):
        return down_even(reach + POST_SWEEPS) + 2 * (COARSE_SWEEPS - 1) + PRE_SWEEPS

    return -(-cycle(cycle(0) + 1) // ROWS) * ROWS


def shift_lanes(value, amount):
    return pltpu.roll(value, amount % LANES, 1)


def neighbours(value, reach, edge):
    rows = value.shape[0]
    lane = lax.broadcasted_iota(jnp.int32, value.shape, 1)
    row = lax.broadcasted_iota(jnp.int32, value.shape, 0)
    column = lane % edge
    hop = reach * edge
    up = jnp.where(column < edge - reach, shift_lanes(value, -reach), 0.0)
    down = jnp.where(column >= reach, shift_lanes(value, reach), 0.0)
    ahead = shift_lanes(value, -hop)
    over = jnp.where(row == rows - 1, 0.0, pltpu.roll(ahead, rows - 1, 0))
    north = jnp.where(lane < LANES - hop, ahead, over)
    behind = shift_lanes(value, hop)
    under = jnp.where(row == 0, 0.0, pltpu.roll(behind, 1, 0))
    south = jnp.where(lane >= hop, behind, under)
    return (up + down) + (north + south)


def block_sum(value, edge):
    lane = lax.broadcasted_iota(jnp.int32, value.shape, 1)
    even_z = lane % 2 == 0
    value = value + jnp.where(even_z, shift_lanes(value, -1), shift_lanes(value, 1))
    even_y = (lane // edge) % 2 == 0
    return value + jnp.where(even_y, shift_lanes(value, -edge), shift_lanes(value, edge))


def cycles_kernel(
    depth, edge, tile, scalars, cells, z_out, image_out, again_out, sums_out,
    r_ref, z_ref, t_ref, image_ref, c_ref, e_ref, f_ref,
):
    groups, padded, width = cells.shape
    planes = padded - 2 * depth
    parts = width // LANES
    count, above, under, group = scalars[0], scalars[1], scalars[2], scalars[3]
    first = (depth - above) // ROWS
    live_end = depth + count * edge
    last = (live_end + under) // ROWS
    own_first, own_last = depth // ROWS, live_end // ROWS
    step = OMEGA / 6.0
    coarse_step = OMEGA / 1.5
    half_rows = ROWS // 2

    def at(plane):
        return pl.ds(pl.multiple_of((plane + 1) * tile, ROWS), tile)

    for ref in (r_ref, z_ref, t_ref, image_ref, c_ref, e_ref, f_ref):
        ref[...] = jnp.zeros(ref.shape, jnp.float32)

    for block in range(padded // ROWS):
        low = block * ROWS
        target = low if low < depth + planes else live_end + (low - depth - planes)
        for part in range(groups * parts):
            rows = pl.ds((target + 1) * tile + part, ROWS, stride=tile)
            lanes = slice(part % parts * LANES, (part % parts + 1) * LANES)
            r_ref[rows, :] = cells[part // parts, low : low + ROWS, lanes]

    def sweep(begin, end, size, reach, source, emit):
        def body(block, carry):
            base = block * size
            window = [source[at(base + k), :] for k in range(-1, size + 1)]
            applied = []
            for k in range(size):
                middle = window[k + 1]
                around = neighbours(middle, reach, edge) + (window[k] + window[k + 2])
                applied.append(6.0 * middle - around)
            emit(base, window[1:-1], applied)
            return carry

        lax.fori_loop(begin, end, body, 0)

    def cycle(rhs):
        def first_sweep(base, middle, applied):
            for k in range(ROWS):
                z_ref[at(base + k), :] = step * (2.0 * middle[k] - step * applied[k])

        sweep(first, last, ROWS, 1, rhs, first_sweep)

        def coarsen(base, middle, applied):
            for k in range(half_rows):
                pair = (rhs[at(base + 2 * k), :] - applied[2 * k]) + (
                    rhs[at(base + 2 * k + 1), :] - applied[2 * k + 1]
                )
                c_ref[at(base // 2 + k), :] = 0.125 * block_sum(pair, edge)

        sweep(first, last, ROWS, 1, z_ref, coarsen)

        def coarse_start(base, middle, applied):
            for k in range(half_rows):
                e_ref[at(base + k), :] = coarse_step * (
                    2.0 * middle[k] - (0.25 * coarse_step) * applied[k]
                )

        sweep(first, last, half_rows, 2, c_ref, coarse_start)
        held, spare = e_ref, f_ref
        for index in range(COARSE_SWEEPS - 2):
            final = index == COARSE_SWEEPS - 3

            def coarse_next(base, middle, applied, spare=spare, final=final):
                for k in range(half_rows):
                    value = middle[k] + coarse_step * (
                        c_ref[at(base + k), :] - 0.25 * applied[k]
                    )
                    if final:
                        for fine in (2 * (base + k), 2 * (base + k) + 1):
                            z_ref[at(fine), :] = z_ref[at(fine), :] + value
                    else:
                        spare[at(base + k), :] = value

            sweep(first, last, half_rows, 2, held, coarse_next)
            held, spare = spare, held

        here, there = z_ref, t_ref
        for index in range(POST_SWEEPS):

            def smooth(base, middle, applied, there=there):
                for k in range(ROWS):
                    there[at(base + k), :] = middle[k] + step * (
                        rhs[at(base + k), :] - applied[k]
                    )

            sweep(first, last, ROWS, 1, here, smooth)
            here, there = there, here
        return here

    def store(ref, out):
        for block in range(planes // ROWS):
            for part in range(parts):
                begin = (depth + block * ROWS + 1) * tile + group * parts + part
                value = ref[pl.ds(begin, ROWS, stride=tile), :]
                lanes = slice(part * LANES, (part + 1) * LANES)
                rows = slice(block * ROWS, (block + 1) * ROWS)
                out[rows, lanes] = jnp.where(block * ROWS < count * edge, value, 0.0)

    zero = jnp.zeros((tile, LANES), jnp.float32)
    result = cycle(r_ref)
    store(result, z_out)

    def to_image(base, middle, applied):
        for k in range(ROWS):
            image_ref[at(base + k), :] = applied[k]

    sweep(first, last, ROWS, 1, result, to_image)
    store(image_ref, image_out)

    def first_sums(block, carry):
        rz, curv = carry
        for k in range(ROWS):
            rows = at(block * ROWS + k)
            rz = rz + r_ref[rows, :] * result[rows, :]
            curv = curv + result[rows, :] * image_ref[rows, :]
        return rz, curv

    rz, curv = lax.fori_loop(own_first, own_last, first_sums, (zero, zero))
    again = cycle(image_ref)
    store(again, again_out)

    def last_sum(block, mixed):
        for k in range(ROWS):
            rows = at(block * ROWS + k)
            mixed = mixed + again[rows, :] * image_ref[rows, :]
        return mixed

    mixed = lax.fori_loop(own_first, own_last, last_sum, zero)
    row = lax.broadcasted_iota(jnp.int32, (ROWS, LANES), 0)
    packed = jnp.zeros((ROWS, LANES), jnp.float32)
    for index, value in enumerate((rz, curv, mixed)):
        total = jnp.sum(value, axis=0, keepdims=True)
        packed = jnp.where(row == index, total, packed)
    for peer in range(sums_out.shape[0] // ROWS):
        sums_out[peer * ROWS : (peer + 1) * ROWS, :] = packed


def finish_kernel(sums, r_ref, z_ref, image_ref, again_ref, solution, residual, direction):
    peers = sums.shape[0] // ROWS
    total = sums[:ROWS, :]
    for peer in range(1, peers):
        total = total + sums[peer * ROWS : (peer + 1) * ROWS, :]
    total = jnp.sum(total, axis=1, keepdims=True)
    rz, curv, mixed = total[0:1], total[1:2], total[2:3]
    alpha = rz / curv
    share = mixed / curv
    z = z_ref[...]
    solution[...] = alpha * z
    residual[...] = r_ref[...] - alpha * image_ref[...]
    direction[...] = alpha * (share * z - again_ref[...])


def send(value, hop):
    count = lax.axis_size("sfc")
    pairs = [(i, (i + hop) % count) for i in range(count)]
    return lax.ppermute(value, "sfc", pairs)


def shards(source, layer_counts):
    count = layer_counts[0]
    slots, edge, width = source.shape
    planes = slots * edge
    depth = halo_depth()
    far = depth - edge
    groups, peers = lax.axis_size("grp"), lax.axis_size("sfc")
    tile = groups * width // LANES
    plane = lax.broadcasted_iota(jnp.int32, (planes, 1), 0)
    own = jnp.where(plane < count * edge, source.reshape(planes, width), 0.0)
    mark = jnp.full((ROWS, width), count.astype(jnp.float32))
    padded = jnp.concatenate([jnp.zeros((far, width), jnp.float32), own], axis=0)
    tail = lax.dynamic_slice_in_dim(padded, count * edge - edge, depth, 0)
    far_tail = lax.dynamic_slice_in_dim(own, count * edge - far, far, 0)
    from_back = send(jnp.concatenate([tail, mark], axis=0), 1)
    from_front = send(jnp.concatenate([own[:depth], mark], axis=0), -1)
    from_far_back = send(far_tail, 2)
    from_far_front = send(own[:far], -2)
    back_count, front_count = from_back[depth, 0], from_front[depth, 0]
    index = lax.axis_index("sfc")
    back_thin, front_thin = back_count < 1.5, front_count < 1.5
    back, front = index > 0, index < peers - 1
    far_back = jnp.where(index > 1, from_far_back, 0.0)
    far_front = jnp.where(index < peers - 2, from_far_front, 0.0)
    cells = jnp.concatenate(
        [
            jnp.where(back, jnp.where(back_thin, far_back, from_back[:far]), 0.0),
            jnp.where(back, from_back[far:depth], 0.0),
            own,
            jnp.where(front, from_front[:edge], 0.0),
            jnp.where(front, jnp.where(front_thin, far_front, from_front[edge:depth]), 0.0),
        ],
        axis=0,
    )
    above = jnp.where((index == 1) & back_thin, edge, depth)
    above = jnp.where(index == 0, 0, above)
    under = jnp.where((index == peers - 2) & front_thin, edge, depth)
    under = jnp.where(index == peers - 1, 0, under)
    scalars = jnp.stack([count, above, under, lax.axis_index("grp")]).astype(jnp.int32)
    gathered = lax.all_gather(cells, "grp", axis=0, tiled=False)
    fine = pltpu.VMEM(((planes + 2 * depth + 2) * tile, LANES), jnp.float32)
    coarse = pltpu.VMEM(((planes // 2 + depth + 2) * tile, LANES), jnp.float32)
    block = jax.ShapeDtypeStruct((planes, width), jnp.float32)
    vmem = pl.BlockSpec(memory_space=pltpu.VMEM)
    z, image, again, sums = pl.pallas_call(
        functools.partial(cycles_kernel, depth, edge, tile),
        out_shape=[block, block, block, jax.ShapeDtypeStruct((peers * ROWS, LANES), jnp.float32)],
        in_specs=[pl.BlockSpec(memory_space=pltpu.SMEM), vmem],
        out_specs=[vmem] * 4,
        scratch_shapes=[fine, fine, fine, fine, coarse, coarse, coarse],
    )(scalars, gathered)
    sums = lax.all_to_all(sums, "sfc", 0, 0, tiled=True)
    outs = pl.pallas_call(
        finish_kernel,
        out_shape=[block] * 3,
        in_specs=[vmem] * 5,
        out_specs=[vmem] * 3,
    )(sums, own, z, image, again)
    return tuple(out.reshape(slots, edge, width) for out in outs)


def solution(mesh):
    return jax.shard_map(
        shards,
        mesh=mesh,
        in_specs=(P("sfc", None, "grp"), P("sfc")),
        out_specs=(P("sfc", None, "grp"), P("sfc", None, "grp"), P("sfc", None, "grp")),
        check_vma=False,
    )
```

```python
import functools

import jax
import jax.numpy as jnp
from jax import lax
from jax.experimental import pallas as pl
from jax.experimental.pallas import tpu as pltpu
from jax.sharding import PartitionSpec as P

PRE_SWEEPS = 2
POST_SWEEPS = 2
COARSE_SWEEPS = 4
OMEGA = 2.0 / 3.0
LANES = 128
ROWS = 8
SPAN = 16


def halo_depth():
    def down_even(plane):
        return plane + plane % 2

    def cycle(reach):
        return down_even(reach + POST_SWEEPS) + 2 * (COARSE_SWEEPS - 1) + PRE_SWEEPS

    return -(-cycle(cycle(0) + 1) // ROWS) * ROWS


def shift_lanes(value, amount):
    return pltpu.roll(value, amount % LANES, 1)


def neighbours(value, next_row, last_row, reach, edge):
    rows = value.shape[0]
    lane = lax.broadcasted_iota(jnp.int32, value.shape, 1)
    row = lax.broadcasted_iota(jnp.int32, value.shape, 0)
    column = lane % edge
    hop = reach * edge
    up = jnp.where(column < edge - reach, shift_lanes(value, -reach), 0.0)
    down = jnp.where(column >= reach, shift_lanes(value, reach), 0.0)
    low = lane < hop
    ahead = jnp.where(low, next_row, value)
    north = shift_lanes(jnp.where(low & (row == rows - 1), 0.0, ahead), -hop)
    high = lane >= LANES - hop
    behind = jnp.where(high, last_row, value)
    south = shift_lanes(jnp.where(high & (row == 0), 0.0, behind), hop)
    return (up + down) + (north + south)


def block_sum(value, edge):
    lane = lax.broadcasted_iota(jnp.int32, value.shape, 1)
    even_z = lane % 2 == 0
    value = value + jnp.where(even_z, shift_lanes(value, -1), shift_lanes(value, 1))
    even_y = (lane // edge) % 2 == 0
    return value + jnp.where(even_y, shift_lanes(value, -edge), shift_lanes(value, edge))


def cycles_kernel(
    depth, edge, tile, scalars, back_mark, front_mark, cells, z_out, image_out, again_out, sums_out,
    r_ref, z_ref, t_ref, image_ref, c_ref, e_ref, f_ref,
):
    groups, padded, width = cells.shape
    planes = padded - 2 * depth
    parts = width // LANES
    count, group, index, peers = scalars[0], scalars[1], scalars[2], scalars[3]
    back_thin = jnp.max(back_mark[...]) < 1.5
    front_thin = jnp.max(front_mark[...]) < 1.5
    above = jnp.where((index == 1) & back_thin, edge, depth)
    above = jnp.where(index == 0, 0, above)
    under = jnp.where((index == peers - 2) & front_thin, edge, depth)
    under = jnp.where(index == peers - 1, 0, under)
    live_end = depth + count * edge
    first, last = depth - above, live_end + under
    step = OMEGA / 6.0
    coarse_step = OMEGA / 1.5

    def at(plane, shift=0):
        start = pl.multiple_of((plane + 1) * tile, ROWS)
        return pl.ds(start + shift if shift else start, tile)

    zero = jnp.zeros((tile, LANES), jnp.float32)
    for ref in (r_ref, z_ref, t_ref, image_ref):
        ref[at(first - 1), :] = zero
        ref[at(last), :] = zero
    for ref in (c_ref, e_ref, f_ref):
        ref[at(first // 2 - 1), :] = zero
        ref[at(last // 2), :] = zero

    for block in range(padded // ROWS):
        low = block * ROWS
        target = low if low < depth + planes else live_end + (low - depth - planes)
        for part in range(groups * parts):
            rows = pl.ds((target + 1) * tile + part, ROWS, stride=tile)
            lanes = slice(part % parts * LANES, (part % parts + 1) * LANES)
            r_ref[rows, :] = cells[part // parts, low : low + ROWS, lanes]

    def sweep(reach, scale, around_of, emit):
        low = jnp.maximum(first, depth - reach) // scale
        high = jnp.minimum(last, live_end + reach) // scale
        size = SPAN // scale

        def body(block, carry):
            base = jnp.minimum(low + block * size, high - size)
            window = [around_of[at(base + k), :] for k in range(-1, size + 1)]
            around = []
            for k in range(size):
                flat = neighbours(
                    window[k + 1],
                    around_of[at(base + k, 1), :],
                    around_of[at(base + k, -1), :],
                    scale,
                    edge,
                )
                around.append(flat + (window[k] + window[k + 2]))
            emit(base, window[1:-1], around)
            return carry

        lax.fori_loop(0, (high - low + size - 1) // size, body, 0)

    def cycle(rhs, reach):
        smooth_reach = reach + POST_SWEEPS + (reach + POST_SWEEPS) % 2
        coarse_reach = smooth_reach + 2 * (COARSE_SWEEPS - 1)

        def first_sweep(base, middle, around):
            for k in range(SPAN):
                z_ref[at(base + k), :] = (step * (2.0 - OMEGA)) * middle[k] + (
                    step * step
                ) * around[k]

        sweep(coarse_reach + 1, 1, rhs, first_sweep)

        def coarsen(base, middle, around):
            defect = [rhs[at(base + k), :] - 6.0 * middle[k] + around[k] for k in range(SPAN)]
            for k in range(SPAN // 2):
                pair = defect[2 * k] + defect[2 * k + 1]
                c_ref[at(base // 2 + k), :] = 0.125 * block_sum(pair, edge)

        sweep(coarse_reach, 1, z_ref, coarsen)

        keep = 1.0 - 1.5 * coarse_step
        spread = 0.25 * coarse_step

        def coarse_start(base, middle, around):
            for k in range(SPAN // 2):
                e_ref[at(base + k), :] = (coarse_step * (1.0 + keep)) * middle[k] + (
                    spread * coarse_step
                ) * around[k]

        sweep(coarse_reach - 2, 2, c_ref, coarse_start)
        held, spare = e_ref, f_ref
        for index in range(COARSE_SWEEPS - 2):
            final = index == COARSE_SWEEPS - 3

            def coarse_next(base, middle, around, spare=spare, final=final):
                for k in range(SPAN // 2):
                    value = (keep * middle[k] + spread * around[k]) + coarse_step * c_ref[at(base + k), :]
                    if final:
                        for fine in (2 * (base + k), 2 * (base + k) + 1):
                            t_ref[at(fine), :] = z_ref[at(fine), :] + value
                    else:
                        spare[at(base + k), :] = value

            sweep(coarse_reach - 4 - 2 * index, 2, held, coarse_next)
            held, spare = spare, held

        here, there = t_ref, z_ref
        for index in range(POST_SWEEPS):

            def smooth(base, middle, around, there=there):
                for k in range(SPAN):
                    there[at(base + k), :] = (1.0 - OMEGA) * middle[k] + step * (
                        rhs[at(base + k), :] + around[k]
                    )

            sweep(reach + POST_SWEEPS - 1 - index, 1, here, smooth)
            here, there = there, here
        return here

    def store(ref, out):
        for block in range(planes // ROWS):
            for part in range(parts):
                begin = (depth + block * ROWS + 1) * tile + group * parts + part
                value = ref[pl.ds(begin, ROWS, stride=tile), :]
                lanes = slice(part * LANES, (part + 1) * LANES)
                rows = slice(block * ROWS, (block + 1) * ROWS)
                out[rows, lanes] = jnp.where(block * ROWS < count * edge, value, 0.0)

    again_reach = 2 * (POST_SWEEPS - POST_SWEEPS // 2) + 2 * (COARSE_SWEEPS - 1) + PRE_SWEEPS
    result = cycle(r_ref, again_reach + 1)
    store(result, z_out)

    def to_image(base, middle, around):
        for k in range(SPAN):
            image_ref[at(base + k), :] = 6.0 * middle[k] - around[k]

    sweep(again_reach, 1, result, to_image)
    store(image_ref, image_out)

    own_first, own_last = depth // ROWS, live_end // ROWS

    def first_sums(block, carry):
        rz, curv = carry
        for k in range(ROWS):
            rows = at(block * ROWS + k)
            rz = rz + r_ref[rows, :] * result[rows, :]
            curv = curv + result[rows, :] * image_ref[rows, :]
        return rz, curv

    rz, curv = lax.fori_loop(own_first, own_last, first_sums, (zero, zero))
    again = cycle(image_ref, 0)
    store(again, again_out)

    def last_sum(block, mixed):
        for k in range(ROWS):
            rows = at(block * ROWS + k)
            mixed = mixed + again[rows, :] * image_ref[rows, :]
        return mixed

    mixed = lax.fori_loop(own_first, own_last, last_sum, zero)
    row = lax.broadcasted_iota(jnp.int32, (ROWS, LANES), 0)
    packed = jnp.zeros((ROWS, LANES), jnp.float32)
    for index, value in enumerate((rz, curv, mixed)):
        total = jnp.sum(value, axis=0, keepdims=True)
        packed = jnp.where(row == index, total, packed)
    for peer in range(sums_out.shape[0] // ROWS):
        sums_out[peer * ROWS : (peer + 1) * ROWS, :] = packed


def finish_kernel(sums, r_ref, z_ref, image_ref, again_ref, solution, residual, direction):
    peers = sums.shape[0] // ROWS
    total = sums[:ROWS, :]
    for peer in range(1, peers):
        total = total + sums[peer * ROWS : (peer + 1) * ROWS, :]
    total = jnp.sum(total, axis=1, keepdims=True)
    rz, curv, mixed = total[0:1], total[1:2], total[2:3]
    alpha = rz / curv
    share = mixed / curv
    z = z_ref[...]
    solution[...] = alpha * z
    residual[...] = r_ref[...] - alpha * image_ref[...]
    direction[...] = alpha * (share * z - again_ref[...])


def send(value, hop):
    count = lax.axis_size("sfc")
    pairs = [(i, (i + hop) % count) for i in range(count)]
    return lax.ppermute(value, "sfc", pairs)


def shards(source, layer_counts):
    count = layer_counts[0]
    slots, edge, width = source.shape
    planes = slots * edge
    depth = halo_depth()
    far = depth - edge
    groups, peers = lax.axis_size("grp"), lax.axis_size("sfc")
    tile = groups * width // LANES
    plane = lax.broadcasted_iota(jnp.int32, (planes, 1), 0)
    own = jnp.where(plane < count * edge, source.reshape(planes, width), 0.0)
    mark = jnp.full((ROWS, width), count.astype(jnp.float32))
    padded = jnp.concatenate([jnp.zeros((far, width), jnp.float32), own], axis=0)
    tail = lax.dynamic_slice_in_dim(padded, count * edge - edge, depth, 0)
    far_tail = lax.dynamic_slice_in_dim(own, count * edge - far, far, 0)
    from_back = send(jnp.concatenate([tail, mark], axis=0), 1)
    from_front = send(jnp.concatenate([own[:depth], mark], axis=0), -1)
    from_far_back = send(far_tail, 2)
    from_far_front = send(own[:far], -2)
    back_mark, front_mark = from_back[depth:], from_front[depth:]
    index = lax.axis_index("sfc")
    back_thin, front_thin = back_mark[:1] < 1.5, front_mark[:1] < 1.5
    back, front = index > 0, index < peers - 1
    far_back = jnp.where(index > 1, from_far_back, 0.0)
    far_front = jnp.where(index < peers - 2, from_far_front, 0.0)
    cells = jnp.concatenate(
        [
            jnp.where(back, jnp.where(back_thin, far_back, from_back[:far]), 0.0),
            jnp.where(back, from_back[far:depth], 0.0),
            own,
            jnp.where(front, from_front[:edge], 0.0),
            jnp.where(front, jnp.where(front_thin, far_front, from_front[edge:depth]), 0.0),
        ],
        axis=0,
    )
    scalars = jnp.stack([count, lax.axis_index("grp"), index, jnp.int32(peers)]).astype(jnp.int32)
    gathered = lax.all_gather(cells, "grp", axis=0, tiled=False)
    fine = pltpu.VMEM(((planes + 2 * depth + 2) * tile, LANES), jnp.float32)
    coarse = pltpu.VMEM(((planes // 2 + depth + 2) * tile, LANES), jnp.float32)
    block = jax.ShapeDtypeStruct((planes, width), jnp.float32)
    vmem = pl.BlockSpec(memory_space=pltpu.VMEM)
    z, image, again, sums = pl.pallas_call(
        functools.partial(cycles_kernel, depth, edge, tile),
        out_shape=[block, block, block, jax.ShapeDtypeStruct((peers * ROWS, LANES), jnp.float32)],
        in_specs=[pl.BlockSpec(memory_space=pltpu.SMEM)] + [vmem] * 3,
        out_specs=[vmem] * 4,
        scratch_shapes=[fine, fine, fine, fine, coarse, coarse, coarse],
    )(scalars, back_mark, front_mark, gathered)
    sums = lax.all_to_all(sums, "sfc", 0, 0, tiled=True)
    outs = pl.pallas_call(
        finish_kernel,
        out_shape=[block] * 3,
        in_specs=[vmem] * 5,
        out_specs=[vmem] * 3,
    )(sums, own, z, image, again)
    return tuple(out.reshape(slots, edge, width) for out in outs)


def solution(mesh):
    return jax.shard_map(
        shards,
        mesh=mesh,
        in_specs=(P("sfc", None, "grp"), P("sfc")),
        out_specs=(P("sfc", None, "grp"), P("sfc", None, "grp"), P("sfc", None, "grp")),
        check_vma=False,
    )
```

```python
import functools

import jax
import jax.numpy as jnp
from jax import lax
from jax.experimental import pallas as pl
from jax.experimental.pallas import tpu as pltpu
from jax.sharding import PartitionSpec as P

PRE_SWEEPS = 2
POST_SWEEPS = 2
COARSE_SWEEPS = 4
OMEGA = 2.0 / 3.0
LANES = 128
ROWS = 8
SPAN = 32
COARSE_SPAN = 8


def halo_depth():
    def down_even(plane):
        return plane + plane % 2

    def cycle(reach):
        return down_even(reach + POST_SWEEPS) + 2 * (COARSE_SWEEPS - 1) + PRE_SWEEPS

    return -(-cycle(cycle(0) + 1) // ROWS) * ROWS


def shift_lanes(value, amount):
    return pltpu.roll(value, amount % LANES, 1)


def neighbours(value, next_row, last_row, reach, edge):
    rows = value.shape[0]
    lane = lax.broadcasted_iota(jnp.int32, value.shape, 1)
    row = lax.broadcasted_iota(jnp.int32, value.shape, 0)
    column = lane % edge
    hop = reach * edge
    up = jnp.where(column < edge - reach, shift_lanes(value, -reach), 0.0)
    down = jnp.where(column >= reach, shift_lanes(value, reach), 0.0)
    low = lane < hop
    ahead = jnp.where(low, next_row, value)
    north = shift_lanes(jnp.where(low & (row == rows - 1), 0.0, ahead), -hop)
    high = lane >= LANES - hop
    behind = jnp.where(high, last_row, value)
    south = shift_lanes(jnp.where(high & (row == 0), 0.0, behind), hop)
    return (up + down) + (north + south)


def inside_matrix(reach, edge):
    source = lax.broadcasted_iota(jnp.int32, (LANES, LANES), 0)
    target = lax.broadcasted_iota(jnp.int32, (LANES, LANES), 1)
    gap = jnp.abs(source - target)
    along_z = (gap == reach) & (source // edge == target // edge)
    return jnp.where(along_z | (gap == reach * edge), 1.0, 0.0).astype(jnp.bfloat16)


def inside_sum(value, matrix):
    high = value.astype(jnp.bfloat16)
    rest = value - high.astype(jnp.float32)
    middle = rest.astype(jnp.bfloat16)
    low = (rest - middle.astype(jnp.float32)).astype(jnp.bfloat16)
    parts = jnp.concatenate([high, middle, low], axis=1)
    return jnp.dot(parts, matrix, preferred_element_type=jnp.float32)


def crossing(next_row, last_row, reach, edge):
    rows = next_row.shape[0]
    lane = lax.broadcasted_iota(jnp.int32, next_row.shape, 1)
    row = lax.broadcasted_iota(jnp.int32, next_row.shape, 0)
    hop = reach * edge
    ahead = jnp.where((lane < hop) & (row < rows - 1), next_row, 0.0)
    behind = jnp.where((lane >= LANES - hop) & (row > 0), last_row, 0.0)
    return shift_lanes(ahead, -hop) + shift_lanes(behind, hop)


def block_sum(value, edge):
    lane = lax.broadcasted_iota(jnp.int32, value.shape, 1)
    even_z = lane % 2 == 0
    value = value + jnp.where(even_z, shift_lanes(value, -1), shift_lanes(value, 1))
    even_y = (lane // edge) % 2 == 0
    return value + jnp.where(even_y, shift_lanes(value, -edge), shift_lanes(value, edge))


def cycles_kernel(
    depth, edge, tile, scalars, back_mark, front_mark, cells, z_out, image_out, again_out, sums_out,
    r_ref, z_ref, t_ref, image_ref, c_ref, e_ref, f_ref, matrix_ref,
):
    groups, padded, width = cells.shape
    planes = padded - 2 * depth
    parts = width // LANES
    count, group, index, peers = scalars[0], scalars[1], scalars[2], scalars[3]
    back_thin = jnp.max(back_mark[...]) > 0.5
    front_thin = jnp.max(front_mark[...]) > 0.5
    above = jnp.where((index == 1) & back_thin, edge, depth)
    above = jnp.where(index == 0, 0, above)
    under = jnp.where((index == peers - 2) & front_thin, edge, depth)
    under = jnp.where(index == peers - 1, 0, under)
    live_end = depth + count * edge
    first, last = depth - above, live_end + under
    step = OMEGA / 6.0
    coarse_step = OMEGA / 1.5
    matrix_ref[...] = jnp.concatenate([inside_matrix(1, edge)] * 3, axis=0)

    def at(plane, shift=0):
        start = pl.multiple_of((plane + 1) * tile, ROWS)
        return pl.ds(start + shift if shift else start, tile)

    zero = jnp.zeros((tile, LANES), jnp.float32)
    for ref in (r_ref, z_ref, t_ref, image_ref):
        ref[at(first - 1), :] = zero
        ref[at(last), :] = zero
    for ref in (c_ref, e_ref, f_ref):
        ref[at(first // 2 - 1), :] = zero
        ref[at(last // 2), :] = zero

    for block in range(padded // ROWS):
        low = block * ROWS
        target = low if low < depth + planes else live_end + (low - depth - planes)
        for part in range(groups * parts):
            rows = pl.ds((target + 1) * tile + part, ROWS, stride=tile)
            lanes = slice(part % parts * LANES, (part % parts + 1) * LANES)
            r_ref[rows, :] = cells[part // parts, low : low + ROWS, lanes]

    def sweep(reach, scale, around_of, emit):
        low = jnp.maximum(first, depth - reach) // scale
        high = jnp.minimum(last, live_end + reach) // scale
        size = SPAN if scale == 1 else COARSE_SPAN

        def body(block, carry):
            base = jnp.maximum(jnp.minimum(low + block * size, high - size), first // scale)
            window = [around_of[at(base + k), :] for k in range(-1, size + 1)]
            if scale == 1:
                whole = around_of[pl.ds(pl.multiple_of((base + 1) * tile, ROWS), size * tile), :]
                inside = inside_sum(whole, matrix_ref[...])
            around = []
            for k in range(size):
                rows_next, rows_last = around_of[at(base + k, 1), :], around_of[at(base + k, -1), :]
                if scale == 1:
                    flat = inside[k * tile : (k + 1) * tile] + crossing(rows_next, rows_last, 1, edge)
                else:
                    flat = neighbours(window[k + 1], rows_next, rows_last, scale, edge)
                around.append(flat + (window[k] + window[k + 2]))
            emit(base, window[1:-1], around)
            return carry

        lax.fori_loop(0, (high - low + size - 1) // size, body, 0)

    def cycle(rhs, reach):
        smooth_reach = reach + POST_SWEEPS + (reach + POST_SWEEPS) % 2
        coarse_reach = smooth_reach + 2 * (COARSE_SWEEPS - 1)

        def first_sweep(base, middle, around):
            for k in range(SPAN):
                z_ref[at(base + k), :] = (step * (2.0 - OMEGA)) * middle[k] + (
                    step * step
                ) * around[k]

        sweep(coarse_reach + 1, 1, rhs, first_sweep)

        def coarsen(base, middle, around):
            defect = [rhs[at(base + k), :] - 6.0 * middle[k] + around[k] for k in range(SPAN)]
            for k in range(SPAN // 2):
                pair = defect[2 * k] + defect[2 * k + 1]
                c_ref[at(base // 2 + k), :] = 0.125 * block_sum(pair, edge)

        sweep(coarse_reach, 1, z_ref, coarsen)

        keep = 1.0 - 1.5 * coarse_step
        spread = 0.25 * coarse_step

        def coarse_start(base, middle, around):
            for k in range(COARSE_SPAN):
                e_ref[at(base + k), :] = (coarse_step * (1.0 + keep)) * middle[k] + (
                    spread * coarse_step
                ) * around[k]

        sweep(coarse_reach - 2, 2, c_ref, coarse_start)
        held, spare = e_ref, f_ref
        for index in range(COARSE_SWEEPS - 2):
            final = index == COARSE_SWEEPS - 3

            def coarse_next(base, middle, around, spare=spare, final=final):
                for k in range(COARSE_SPAN):
                    value = (keep * middle[k] + spread * around[k]) + coarse_step * c_ref[at(base + k), :]
                    if final:
                        for fine in (2 * (base + k), 2 * (base + k) + 1):
                            t_ref[at(fine), :] = z_ref[at(fine), :] + value
                    else:
                        spare[at(base + k), :] = value

            sweep(coarse_reach - 4 - 2 * index, 2, held, coarse_next)
            held, spare = spare, held

        here, there = t_ref, z_ref
        for index in range(POST_SWEEPS):

            def smooth(base, middle, around, there=there):
                for k in range(SPAN):
                    there[at(base + k), :] = (1.0 - OMEGA) * middle[k] + step * (
                        rhs[at(base + k), :] + around[k]
                    )

            sweep(reach + POST_SWEEPS - 1 - index, 1, here, smooth)
            here, there = there, here
        return here

    def store(ref, out):
        for block in range(planes // ROWS):
            for part in range(parts):
                begin = (depth + block * ROWS + 1) * tile + group * parts + part
                value = ref[pl.ds(begin, ROWS, stride=tile), :]
                lanes = slice(part * LANES, (part + 1) * LANES)
                rows = slice(block * ROWS, (block + 1) * ROWS)
                out[rows, lanes] = jnp.where(block * ROWS < count * edge, value, 0.0)

    again_reach = 2 * (POST_SWEEPS - POST_SWEEPS // 2) + 2 * (COARSE_SWEEPS - 1) + PRE_SWEEPS
    result = cycle(r_ref, again_reach + 1)
    store(result, z_out)

    def to_image(base, middle, around):
        for k in range(SPAN):
            image_ref[at(base + k), :] = 6.0 * middle[k] - around[k]

    sweep(again_reach, 1, result, to_image)
    store(image_ref, image_out)

    own_first, own_last = depth // ROWS, live_end // ROWS

    def first_sums(block, carry):
        rz, curv = carry
        for k in range(ROWS):
            rows = at(block * ROWS + k)
            rz = rz + r_ref[rows, :] * result[rows, :]
            curv = curv + result[rows, :] * image_ref[rows, :]
        return rz, curv

    rz, curv = lax.fori_loop(own_first, own_last, first_sums, (zero, zero))
    again = cycle(image_ref, 0)
    store(again, again_out)

    def last_sum(block, mixed):
        for k in range(ROWS):
            rows = at(block * ROWS + k)
            mixed = mixed + again[rows, :] * image_ref[rows, :]
        return mixed

    mixed = lax.fori_loop(own_first, own_last, last_sum, zero)
    row = lax.broadcasted_iota(jnp.int32, (ROWS, LANES), 0)
    packed = jnp.zeros((ROWS, LANES), jnp.float32)
    for index, value in enumerate((rz, curv, mixed)):
        total = jnp.sum(value, axis=0, keepdims=True)
        packed = jnp.where(row == index, total, packed)
    for peer in range(sums_out.shape[0] // ROWS):
        sums_out[peer * ROWS : (peer + 1) * ROWS, :] = packed


def finish_kernel(sums, r_ref, z_ref, image_ref, again_ref, solution, residual, direction):
    peers = sums.shape[0] // ROWS
    total = sums[:ROWS, :]
    for peer in range(1, peers):
        total = total + sums[peer * ROWS : (peer + 1) * ROWS, :]
    total = jnp.sum(total, axis=1, keepdims=True)
    rz, curv, mixed = total[0:1], total[1:2], total[2:3]
    alpha = rz / curv
    share = mixed / curv
    z = z_ref[...]
    solution[...] = alpha * z
    residual[...] = r_ref[...] - alpha * image_ref[...]
    direction[...] = alpha * (share * z - again_ref[...])


def send(value, hop):
    count = lax.axis_size("sfc")
    pairs = [(i, (i + hop) % count) for i in range(count)]
    return lax.ppermute(value, "sfc", pairs)


def shards(source, layer_counts):
    count = layer_counts[0]
    slots, edge, width = source.shape
    planes = slots * edge
    depth = halo_depth()
    far = depth - edge
    groups, peers = lax.axis_size("grp"), lax.axis_size("sfc")
    tile = groups * width // LANES
    plane = lax.broadcasted_iota(jnp.int32, (planes, 1), 0)
    own = jnp.where(plane < count * edge, source.reshape(planes, width), 0.0)
    mark = jnp.full((far, width), jnp.where(count == 1, 1.0, 0.0).astype(jnp.float32))
    padded = jnp.concatenate([jnp.zeros((far, width), jnp.float32), own], axis=0)
    tail = lax.dynamic_slice_in_dim(padded, count * edge - edge, depth, 0)
    far_tail = lax.dynamic_slice_in_dim(own, count * edge - far, far, 0)
    from_back = send(jnp.concatenate([tail, mark], axis=0), 1)
    from_front = send(jnp.concatenate([own[:depth], mark], axis=0), -1)
    from_far_back = send(far_tail, 2)
    from_far_front = send(own[:far], -2)
    back_mark, front_mark = from_back[depth:], from_front[depth:]
    index = lax.axis_index("sfc")
    back, front = index > 0, index < peers - 1
    far_back = jnp.where(index > 1, from_far_back, 0.0)
    far_front = jnp.where(index < peers - 2, from_far_front, 0.0)
    cells = jnp.concatenate(
        [
            jnp.where(back, from_back[:far] + back_mark * far_back, 0.0),
            jnp.where(back, from_back[far:depth], 0.0),
            own,
            jnp.where(front, from_front[:edge], 0.0),
            jnp.where(front, from_front[edge:depth] + front_mark * far_front, 0.0),
        ],
        axis=0,
    )
    scalars = jnp.stack([count, lax.axis_index("grp"), index, jnp.int32(peers)]).astype(jnp.int32)
    gathered = lax.all_gather(cells, "grp", axis=0, tiled=False)
    fine = pltpu.VMEM(((planes + 2 * depth + 2) * tile, LANES), jnp.float32)
    coarse = pltpu.VMEM(((planes // 2 + depth + 2) * tile, LANES), jnp.float32)
    block = jax.ShapeDtypeStruct((planes, width), jnp.float32)
    vmem = pl.BlockSpec(memory_space=pltpu.VMEM)
    z, image, again, sums = pl.pallas_call(
        functools.partial(cycles_kernel, depth, edge, tile),
        out_shape=[block, block, block, jax.ShapeDtypeStruct((peers * ROWS, LANES), jnp.float32)],
        in_specs=[pl.BlockSpec(memory_space=pltpu.SMEM)] + [vmem] * 3,
        out_specs=[vmem] * 4,
        scratch_shapes=[fine, fine, fine, fine, coarse, coarse, coarse]
        + [pltpu.VMEM((3 * LANES, LANES), jnp.bfloat16)],
    )(scalars, back_mark, front_mark, gathered)
    sums = lax.all_to_all(sums, "sfc", 0, 0, tiled=True)
    outs = pl.pallas_call(
        finish_kernel,
        out_shape=[block] * 3,
        in_specs=[vmem] * 5,
        out_specs=[vmem] * 3,
    )(sums, own, z, image, again)
    return tuple(out.reshape(slots, edge, width) for out in outs)


def solution(mesh):
    return jax.shard_map(
        shards,
        mesh=mesh,
        in_specs=(P("sfc", None, "grp"), P("sfc")),
        out_specs=(P("sfc", None, "grp"), P("sfc", None, "grp"), P("sfc", None, "grp")),
        check_vma=False,
    )
```

```python
import functools

import jax
import jax.numpy as jnp
from jax import lax
from jax.experimental import pallas as pl
from jax.experimental.pallas import tpu as pltpu
from jax.sharding import PartitionSpec as P

PRE_SWEEPS = 2
POST_SWEEPS = 2
COARSE_SWEEPS = 4
OMEGA = 2.0 / 3.0
LANES = 128
ROWS = 8
SPAN = 32
COARSE_SPAN = 8


def halo_depth():
    def down_even(plane):
        return plane + plane % 2

    def cycle(reach):
        return down_even(reach + POST_SWEEPS) + 2 * (COARSE_SWEEPS - 1) + PRE_SWEEPS

    return -(-cycle(cycle(0) + 1) // ROWS) * ROWS


def shift_lanes(value, amount):
    return pltpu.roll(value, amount % LANES, 1)


def neighbours(value, next_row, last_row, reach, edge):
    rows = value.shape[0]
    lane = lax.broadcasted_iota(jnp.int32, value.shape, 1)
    row = lax.broadcasted_iota(jnp.int32, value.shape, 0)
    column = lane % edge
    hop = reach * edge
    up = jnp.where(column < edge - reach, shift_lanes(value, -reach), 0.0)
    down = jnp.where(column >= reach, shift_lanes(value, reach), 0.0)
    low = lane < hop
    ahead = jnp.where(low, next_row, value)
    north = shift_lanes(jnp.where(low & (row == rows - 1), 0.0, ahead), -hop)
    high = lane >= LANES - hop
    behind = jnp.where(high, last_row, value)
    south = shift_lanes(jnp.where(high & (row == 0), 0.0, behind), hop)
    return (up + down) + (north + south)


def inside_matrix(reach, edge):
    source = lax.broadcasted_iota(jnp.int32, (LANES, LANES), 0)
    target = lax.broadcasted_iota(jnp.int32, (LANES, LANES), 1)
    gap = jnp.abs(source - target)
    along_z = (gap == reach) & (source // edge == target // edge)
    return jnp.where(along_z | (gap == reach * edge), 1.0, 0.0).astype(jnp.bfloat16)


def inside_sum(value, matrix):
    high = value.astype(jnp.bfloat16)
    rest = value - high.astype(jnp.float32)
    middle = rest.astype(jnp.bfloat16)
    low = (rest - middle.astype(jnp.float32)).astype(jnp.bfloat16)
    parts = jnp.concatenate([high, middle, low], axis=1)
    return jnp.dot(parts, matrix, preferred_element_type=jnp.float32)


def crossing(next_row, last_row, reach, edge):
    rows = next_row.shape[0]
    lane = lax.broadcasted_iota(jnp.int32, next_row.shape, 1)
    row = lax.broadcasted_iota(jnp.int32, next_row.shape, 0)
    hop = reach * edge
    ahead = jnp.where((lane < hop) & (row < rows - 1), next_row, 0.0)
    behind = jnp.where((lane >= LANES - hop) & (row > 0), last_row, 0.0)
    return shift_lanes(ahead, -hop) + shift_lanes(behind, hop)


def block_sum(value, edge):
    lane = lax.broadcasted_iota(jnp.int32, value.shape, 1)
    even_z = lane % 2 == 0
    value = value + jnp.where(even_z, shift_lanes(value, -1), shift_lanes(value, 1))
    even_y = (lane // edge) % 2 == 0
    return value + jnp.where(even_y, shift_lanes(value, -edge), shift_lanes(value, edge))


def cycles_kernel(
    depth, edge, tile, scalars, back_mark, front_mark, cells, z_out, image_out, again_out, sums_out,
    r_ref, z_ref, t_ref, image_ref, c_ref, e_ref, f_ref, matrix_ref,
):
    groups, padded, width = cells.shape
    planes = padded - 2 * depth
    parts = width // LANES
    count, group, index, peers = scalars[0], scalars[1], scalars[2], scalars[3]
    back_thin = jnp.max(back_mark[...]) > 0.5
    front_thin = jnp.max(front_mark[...]) > 0.5
    above = jnp.where((index == 1) & back_thin, edge, depth)
    above = jnp.where(index == 0, 0, above)
    under = jnp.where((index == peers - 2) & front_thin, edge, depth)
    under = jnp.where(index == peers - 1, 0, under)
    live_end = depth + count * edge
    first, last = depth - above, live_end + under
    step = OMEGA / 6.0
    coarse_step = OMEGA / 1.5
    matrix_ref[...] = jnp.concatenate([inside_matrix(1, edge)] * 3, axis=0)

    def at(plane, shift=0):
        start = pl.multiple_of((plane + 1) * tile, ROWS)
        return pl.ds(start + shift if shift else start, tile)

    zero = jnp.zeros((tile, LANES), jnp.float32)
    for ref in (r_ref, z_ref, t_ref, image_ref):
        ref[at(first - 1), :] = zero
        ref[at(last), :] = zero
    for ref in (c_ref, e_ref, f_ref):
        ref[at(first // 2 - 1), :] = zero
        ref[at(last // 2), :] = zero

    for block in range(padded // ROWS):
        low = block * ROWS
        target = low if low < depth + planes else live_end + (low - depth - planes)
        for part in range(groups * parts):
            rows = pl.ds((target + 1) * tile + part, ROWS, stride=tile)
            lanes = slice(part % parts * LANES, (part % parts + 1) * LANES)
            r_ref[rows, :] = cells[part // parts, low : low + ROWS, lanes]

    def sweep(reach, scale, around_of, emit):
        low = jnp.maximum(first, depth - reach) // scale
        high = jnp.minimum(last, live_end + reach) // scale
        size = SPAN if scale == 1 else COARSE_SPAN

        def body(block, carry):
            base = jnp.maximum(jnp.minimum(low + block * size, high - size), first // scale)
            window = [around_of[at(base + k), :] for k in range(-1, size + 1)]
            if scale == 1:
                whole = around_of[pl.ds(pl.multiple_of((base + 1) * tile, ROWS), size * tile), :]
                inside = inside_sum(whole, matrix_ref[...])
            around = []
            for k in range(size):
                rows_next, rows_last = around_of[at(base + k, 1), :], around_of[at(base + k, -1), :]
                if scale == 1:
                    flat = inside[k * tile : (k + 1) * tile] + crossing(rows_next, rows_last, 1, edge)
                else:
                    flat = neighbours(window[k + 1], rows_next, rows_last, scale, edge)
                around.append(flat + (window[k] + window[k + 2]))
            emit(base, window[1:-1], around)
            return carry

        lax.fori_loop(0, (high - low + size - 1) // size, body, 0)

    def cycle(rhs, reach):
        smooth_reach = reach + POST_SWEEPS + (reach + POST_SWEEPS) % 2
        coarse_reach = smooth_reach + 2 * (COARSE_SWEEPS - 1)

        def first_sweep(base, middle, around):
            for k in range(SPAN):
                z_ref[at(base + k), :] = (step * (2.0 - OMEGA)) * middle[k] + (
                    step * step
                ) * around[k]

        sweep(coarse_reach + 1, 1, rhs, first_sweep)

        def coarsen(base, middle, around):
            defect = [rhs[at(base + k), :] - 6.0 * middle[k] + around[k] for k in range(SPAN)]
            for k in range(SPAN // 2):
                pair = defect[2 * k] + defect[2 * k + 1]
                c_ref[at(base // 2 + k), :] = 0.125 * block_sum(pair, edge)

        sweep(coarse_reach, 1, z_ref, coarsen)

        keep = 1.0 - 1.5 * coarse_step
        spread = 0.25 * coarse_step

        def coarse_start(base, middle, around):
            for k in range(COARSE_SPAN):
                e_ref[at(base + k), :] = (coarse_step * (1.0 + keep)) * middle[k] + (
                    spread * coarse_step
                ) * around[k]

        sweep(coarse_reach - 2, 2, c_ref, coarse_start)
        held, spare = e_ref, f_ref
        for index in range(COARSE_SWEEPS - 2):
            final = index == COARSE_SWEEPS - 3

            def coarse_next(base, middle, around, spare=spare, final=final):
                for k in range(COARSE_SPAN):
                    value = (keep * middle[k] + spread * around[k]) + coarse_step * c_ref[at(base + k), :]
                    if final:
                        for fine in (2 * (base + k), 2 * (base + k) + 1):
                            t_ref[at(fine), :] = z_ref[at(fine), :] + value
                    else:
                        spare[at(base + k), :] = value

            sweep(coarse_reach - 4 - 2 * index, 2, held, coarse_next)
            held, spare = spare, held

        here, there = t_ref, z_ref
        for index in range(POST_SWEEPS):

            def smooth(base, middle, around, there=there):
                for k in range(SPAN):
                    there[at(base + k), :] = (1.0 - OMEGA) * middle[k] + step * (
                        rhs[at(base + k), :] + around[k]
                    )

            sweep(reach + POST_SWEEPS - 1 - index, 1, here, smooth)
            here, there = there, here
        return here

    def store(ref, out):
        for block in range(planes // ROWS):
            for part in range(parts):
                begin = (depth + block * ROWS + 1) * tile + group * parts + part
                value = ref[pl.ds(begin, ROWS, stride=tile), :]
                lanes = slice(part * LANES, (part + 1) * LANES)
                rows = slice(block * ROWS, (block + 1) * ROWS)
                out[rows, lanes] = jnp.where(block * ROWS < count * edge, value, 0.0)

    again_reach = 2 * (POST_SWEEPS - POST_SWEEPS // 2) + 2 * (COARSE_SWEEPS - 1) + PRE_SWEEPS
    result = cycle(r_ref, again_reach + 1)
    store(result, z_out)

    def to_image(base, middle, around):
        for k in range(SPAN):
            image_ref[at(base + k), :] = 6.0 * middle[k] - around[k]

    sweep(again_reach, 1, result, to_image)
    store(image_ref, image_out)

    own_first, own_last = depth // ROWS, live_end // ROWS

    def first_sums(block, carry):
        rz, curv = carry
        for k in range(ROWS):
            rows = at(block * ROWS + k)
            rz = rz + r_ref[rows, :] * result[rows, :]
            curv = curv + result[rows, :] * image_ref[rows, :]
        return rz, curv

    rz, curv = lax.fori_loop(own_first, own_last, first_sums, (zero, zero))
    again = cycle(image_ref, 0)
    store(again, again_out)

    def last_sum(block, mixed):
        for k in range(ROWS):
            rows = at(block * ROWS + k)
            mixed = mixed + again[rows, :] * image_ref[rows, :]
        return mixed

    mixed = lax.fori_loop(own_first, own_last, last_sum, zero)
    row = lax.broadcasted_iota(jnp.int32, (ROWS, LANES), 0)
    packed = jnp.zeros((ROWS, LANES), jnp.float32)
    for index, value in enumerate((rz, curv, mixed)):
        total = jnp.sum(value, axis=0, keepdims=True)
        packed = jnp.where(row == index, total, packed)
    for peer in range(sums_out.shape[0] // ROWS):
        sums_out[peer * ROWS : (peer + 1) * ROWS, :] = packed


def finish_kernel(sums, r_ref, z_ref, image_ref, again_ref, solution, residual, direction):
    peers = sums.shape[0] // ROWS
    total = sums[:ROWS, :]
    for peer in range(1, peers):
        total = total + sums[peer * ROWS : (peer + 1) * ROWS, :]
    total = jnp.sum(total, axis=1, keepdims=True)
    rz, curv, mixed = total[0:1], total[1:2], total[2:3]
    alpha = rz / curv
    share = mixed / curv
    z = z_ref[...]
    solution[...] = alpha * z
    residual[...] = r_ref[...] - alpha * image_ref[...]
    direction[...] = alpha * (share * z - again_ref[...])


def send(value, hop):
    count = lax.axis_size("sfc")
    pairs = [(i, (i + hop) % count) for i in range(count)]
    return lax.ppermute(value, "sfc", pairs)


def placed(value, start, total):
    return jnp.pad(value, ((start, total - start - value.shape[0]), (0, 0)))


def shards(source, layer_counts):
    count = layer_counts[0]
    slots, edge, width = source.shape
    planes = slots * edge
    depth = halo_depth()
    far = depth - edge
    groups, peers = lax.axis_size("grp"), lax.axis_size("sfc")
    tile = groups * width // LANES
    plane = lax.broadcasted_iota(jnp.int32, (planes, 1), 0)
    own = jnp.where(plane < count * edge, source.reshape(planes, width), 0.0)
    mark = jnp.full((far, width), jnp.where(count == 1, 1.0, 0.0).astype(jnp.float32))
    padded = jnp.concatenate([jnp.zeros((far, width), jnp.float32), own], axis=0)
    tail = lax.dynamic_slice_in_dim(padded, count * edge - edge, depth, 0)
    far_tail = lax.dynamic_slice_in_dim(own, count * edge - far, far, 0)
    from_back = send(placed(tail, 0, depth + far) + placed(mark, depth, depth + far), 1)
    from_front = send(placed(own[:depth], 0, depth + far) + placed(mark, depth, depth + far), -1)
    from_far_back = send(far_tail, 2)
    from_far_front = send(own[:far], -2)
    back_mark, front_mark = from_back[depth:], from_front[depth:]
    index = lax.axis_index("sfc")
    back, front = index > 0, index < peers - 1
    far_back = jnp.where(index > 1, from_far_back, 0.0)
    far_front = jnp.where(index < peers - 2, from_far_front, 0.0)
    above = jnp.where(back, from_back[:depth] + placed(back_mark * far_back, 0, depth), 0.0)
    below = jnp.where(front, from_front[:depth] + placed(front_mark * far_front, edge, depth), 0.0)
    total = planes + 2 * depth
    cells = placed(own, depth, total) + (placed(above, 0, total) + placed(below, depth + planes, total))
    scalars = jnp.stack([count, lax.axis_index("grp"), index, jnp.int32(peers)]).astype(jnp.int32)
    gathered = lax.all_gather(cells, "grp", axis=0, tiled=False)
    fine = pltpu.VMEM(((planes + 2 * depth + 2) * tile, LANES), jnp.float32)
    coarse = pltpu.VMEM(((planes // 2 + depth + 2) * tile, LANES), jnp.float32)
    block = jax.ShapeDtypeStruct((planes, width), jnp.float32)
    vmem = pl.BlockSpec(memory_space=pltpu.VMEM)
    z, image, again, sums = pl.pallas_call(
        functools.partial(cycles_kernel, depth, edge, tile),
        out_shape=[block, block, block, jax.ShapeDtypeStruct((peers * ROWS, LANES), jnp.float32)],
        in_specs=[pl.BlockSpec(memory_space=pltpu.SMEM)] + [vmem] * 3,
        out_specs=[vmem] * 4,
        scratch_shapes=[fine, fine, fine, fine, coarse, coarse, coarse]
        + [pltpu.VMEM((3 * LANES, LANES), jnp.bfloat16)],
    )(scalars, back_mark, front_mark, gathered)
    sums = lax.all_to_all(sums, "sfc", 0, 0, tiled=True)
    outs = pl.pallas_call(
        finish_kernel,
        out_shape=[block] * 3,
        in_specs=[vmem] * 5,
        out_specs=[vmem] * 3,
    )(sums, own, z, image, again)
    return tuple(out.reshape(slots, edge, width) for out in outs)


def solution(mesh):
    return jax.shard_map(
        shards,
        mesh=mesh,
        in_specs=(P("sfc", None, "grp"), P("sfc")),
        out_specs=(P("sfc", None, "grp"), P("sfc", None, "grp"), P("sfc", None, "grp")),
        check_vma=False,
    )
```
